32 devices in a mesh: tok: 8 (over z, y), voc: 4 (over x, core).
Axes of the slice: x: 2, y: 2, z: 4, core: 2. Of those that a mesh axis runs over, the one named last changes fastest.
Arguments:
- hidden: bfloat16 [1024, 2048], P('tok'), may hold values from -6 to 6
- mix_weight: bfloat16 [4, 2048], P(None, 'voc'), may hold values from -0.0546875 to 0.0546875
- comp_proj: bfloat16 [2048, 4, 2048], P(None, None, 'voc'), may hold values from -0.110485435 to 0.110485435
- vocab_weight: bfloat16 [2048, 1024], P(None, 'voc'), may hold values from -0.625 to 0.625
- log_normalizer: float32 [4, 1024], P(None, 'tok'), may hold values from 11 to 11.6
- targets: int32 [1024], P('tok'), may hold values from 0 to 1023
- loss_grad: float32 [1024], P('tok'), may hold values from 0.5 to 1.5
Outputs:
- hidden_grad: bfloat16 [1024, 2048], P('tok', 'voc')
- proj_grad: bfloat16 [2048, 4, 2048], P('tok', None, 'voc')
- vocab_grad: bfloat16 [2048, 1024], P('tok', 'voc')
The draws below stay inside these ranges and needn't reach their ends.
All inputs are finite; a program needn't handle non-finite values.
Results may differ from the reference program's by a relative error of at most 0.02.
Values may be sent and summed in bfloat16 or wider, within the bound.
A program may use at most 64 MiB of HBM per device.

```python
import jax
import jax.numpy as jnp
from jax import lax

D = 2048
K = 4
TOK_DEV = 128
V_DEV = 256
TOKENS = 1024
VOCAB = 1024
N_TOK = 8
N_VOC = 4


def draw_comp_proj(key, part):
    base_key = jax.random.fold_in(key, 11)
    noise_key = jax.random.fold_in(key, 12)
    shared = jax.random.truncated_normal(base_key, -4.0, 4.0, (D, 1, D), jnp.float32)
    private = jax.random.truncated_normal(noise_key, -4.0, 4.0, (D, K, D), jnp.float32)
    values = (0.98869 * shared + 0.15 * private) * D ** (-0.5)
    return values.astype(jnp.bfloat16)


def set_ends(array, stream_key, low, top_value):
    longest = array.shape.index(max(array.shape))
    spots = []
    for shift in (0, 1):
        where = [jax.random.randint(jax.random.fold_in(stream_key, axis), (), 0, length) for axis, length in enumerate(array.shape)]
        where[longest] = (where[longest] + shift) % array.shape[longest]
        spots.append(tuple(where))
    return array.at[spots[0]].set(low).at[spots[1]].set(top_value)


def level_of(key, shape, cuts, smallest, high):
    def one(position, parts):
        heights = jax.random.uniform(jax.random.fold_in(jax.random.fold_in(key, 6), position), (parts,), jnp.float32, smallest / len(cuts), high / len(cuts))
        return jnp.repeat(jnp.exp(heights), shape[position] // parts).reshape((-1,) + (1,) * (len(shape) - position - 1))

    level = one(*cuts[0])
    for cut in cuts[1:]:
        level = level * one(*cut)
    return level


def noise(key, extent, width, reach, split=(), kind=jnp.bfloat16):
    entries = jax.random.normal(key, extent, jnp.float32) * width
    if len(split) > 0:
        entries = level_of(key, extent, split, -0.22, 0.18) * entries
    return jnp.clip(entries, min=-reach, max=reach).astype(kind)


def setup_inputs(seed: int = 0) -> dict:
    key_of = jax.random.split(jax.random.key(seed), 8)
    hidden = noise(key_of[0], (TOKENS, D), 1.0, 6.0, ((0, 8),))
    mix_weight = noise(key_of[1], (K, D), (6 * D) ** -0.5, 0.0546875, ((1, 4),))
    comp_proj = draw_comp_proj(jax.random.fold_in(key_of[7], 71), 0)
    vocab_weight = noise(key_of[3], (D, VOCAB), 0.1, 0.625, ((1, 4),))
    log_normalizer = jnp.clip(11.0 + 0.6000004 * jax.random.uniform(key_of[4], (K, TOKENS), jnp.float32) ** level_of(key_of[4], (K, TOKENS), ((1, 8),), -0.2, 0.2), 11.0, 11.6)
    targets = set_ends(jax.random.randint(key_of[5], (TOKENS,), 0, VOCAB), jax.random.fold_in(key_of[5], 1), 0, VOCAB - 1).astype(jnp.int32)
    loss_grad = jnp.clip(0.5 + 1.0 * jax.random.uniform(key_of[6], (TOKENS,), jnp.float32) ** level_of(key_of[6], (TOKENS,), ((0, 8),), -0.2, 0.2), 0.5, 1.5)
    return {"hidden": hidden, "mix_weight": mix_weight, "comp_proj": comp_proj, "vocab_weight": vocab_weight, "log_normalizer": log_normalizer, "targets": targets, "loss_grad": loss_grad}


def rounded(values):
    return lax.optimization_barrier(values.astype(jnp.bfloat16)).astype(jnp.float32)


def reference(hidden, mix_weight, comp_proj, vocab_weight, log_normalizer, targets, loss_grad):
    highest = lax.Precision.HIGHEST
    weight_full = vocab_weight.astype(jnp.float32)
    proj_full = comp_proj.astype(jnp.float32)
    mix_full = mix_weight.astype(jnp.float32)
    vocab_ids = jnp.arange(VOCAB, dtype=jnp.int32)
    hidden_groups = hidden.reshape(N_TOK, TOK_DEV, D)
    norm_groups = jnp.transpose(log_normalizer.reshape(K, N_TOK, TOK_DEV), (1, 0, 2))
    target_groups = targets.reshape(N_TOK, TOK_DEV)
    cotangent_groups = loss_grad.reshape(N_TOK, TOK_DEV)

    def one_group(running, inputs):
        vocab_sum, proj_sum = running
        states, normalizer, wanted, cotangent = inputs
        states_f = states.astype(jnp.float32)
        contexts = jnp.tanh(jnp.einsum("td,dke->tke", states_f, proj_full, precision=highest)).astype(jnp.bfloat16)
        context_f = contexts.astype(jnp.float32)
        logits = jnp.einsum("tkd,dv->ktv", context_f, weight_full, precision=highest)
        mixing = jnp.einsum("td,kd->kt", states_f, mix_full, precision=highest)
        onehot = (wanted[:, None] == vocab_ids[None, :]).astype(jnp.float32)
        target = jnp.sum(logits * onehot[None], axis=2)
        exp_mix = jnp.exp(mixing)
        weights = exp_mix / jnp.sum(exp_mix, axis=0, keepdims=True)
        likely = jnp.exp(target - normalizer)
        joint_mass = weights * likely
        posterior = joint_mass / jnp.sum(joint_mass, axis=0, keepdims=True)
        factor = cotangent[None, :] * posterior
        logit_grad = (factor[:, :, None] * (jnp.exp(logits - normalizer[:, :, None]) - onehot[None])).astype(jnp.bfloat16)
        mixing_grad = cotangent[None, :] * (weights - posterior)
        grad_f = logit_grad.astype(jnp.float32)
        vocab_part = jnp.einsum("tkd,ktv->dv", context_f, grad_f, precision=highest)
        vocab_sum = vocab_sum + rounded(vocab_part)
        blocks = jnp.einsum("ktbv,dbv->btkd", grad_f.reshape(K, TOK_DEV, N_VOC, V_DEV), weight_full.reshape(D, N_VOC, V_DEV), precision=highest)
        context_grad = jnp.sum(rounded(blocks), axis=0)
        pre_grad = rounded(context_grad * (1.0 - context_f * context_f))
        hidden_grad = (jnp.einsum("tke,jke->tj", pre_grad, proj_full, precision=highest) + jnp.einsum("kt,kd->td", mixing_grad, mix_full, precision=highest)).astype(jnp.bfloat16)
        proj_sum = proj_sum + jnp.einsum("tj,tke->jke", states_f, pre_grad, precision=highest)
        return (vocab_sum, proj_sum), hidden_grad

    start_state = (jnp.zeros((D, VOCAB), jnp.float32), jnp.zeros((D, K, D), jnp.float32))
    final_state, hidden_grads = lax.scan(one_group, start_state, (hidden_groups, norm_groups, target_groups, cotangent_groups))
    vocab_sum, proj_sum = final_state
    return hidden_grads.reshape(TOKENS, D), proj_sum.astype(jnp.bfloat16), vocab_sum.astype(jnp.bfloat16)
```

```python
import functools

import jax
import jax.numpy as jnp
from jax import lax
from jax.experimental import pallas as pl
from jax.experimental.pallas import tpu as pltpu
from jax.sharding import PartitionSpec as P

MESH = pl.DeviceIdType.MESH
F32 = jnp.float32
BF16 = jnp.bfloat16
NT = (((1,), (1,)), ((), ()))
TN = (((0,), (0,)), ((), ()))


def column(row, lanes):
    wide = jnp.broadcast_to(row, (128, row.shape[1])).T
    return jnp.concatenate([wide] * (lanes // 128), axis=1)


def kernel(
    M, N,
    hidden, mix, proj_hbm, vw, logz, targets, loss,
    out_hidden, out_proj, out_vocab,
    w, ctx, mix_all, hblk, hrow, logit, lg, tgt,
    cgs, cgr, cgx, xr, own_cg, vgb, vgr, pg, hss, hsr, own_hs, acc, mgrad,
    w_sem, ctx_s, ctx_f, ctx_r, mix_s, mix_r, hid_s, hid_r, tgt_s, tgt_r,
    cgp_s, cgp_r, cgx_s, cgx_r, vg_s, vg_r, hs_s, hs_r, ag_s, ag_r,
):
    K, D, E = w.shape
    T = hidden.shape[0]
    V = vw.shape[1]
    R = D // M
    half = N // 2
    Z = M // 2
    me_t = lax.axis_index("tok")
    me_v = lax.axis_index("voc")
    chip = me_v // 2
    core = me_v % 2
    partner = me_v + 1 - 2 * core
    z = me_t // 2
    y = me_t % 2
    ypart = me_t + 1 - 2 * y
    sends = []

    def remote(src, dst, ss, rs, dev):
        return pltpu.make_async_remote_copy(
            src_ref=src, dst_ref=dst, send_sem=ss, recv_sem=rs,
            device_id=dev, device_id_type=MESH,
        )

    def send(src, dst, ss, rs, dev):
        c = remote(src, dst, ss, rs, dev)
        c.start()
        sends.append((None, c))

    def arrived(ref, rs, ss):
        remote(ref, ref, ss, rs, {"voc": partner}).wait_recv()

    for k in range(K):
        pltpu.make_async_copy(proj_hbm.at[k], w.at[k], w_sem.at[k]).start()
    for j in range(M):
        hblk[j] = hidden[:, j * R:(j + 1) * R]

    bar = pltpu.get_barrier_semaphore()
    for d in range(1, M):
        pl.semaphore_signal(bar, inc=1, device_id={"tok": lax.rem(me_t + d, M)}, device_id_type=MESH)
    for d in range(1, N):
        pl.semaphore_signal(bar, inc=1, device_id={"voc": lax.rem(me_v + d, N)}, device_id_type=MESH)
    pl.semaphore_wait(bar, M + N - 2)

    for d in range(1, N):
        send(mix, mix_all.at[d], mix_s.at[d], mix_r.at[d], {"voc": lax.rem(me_v + d, N)})
    mix_all[0] = mix[...]
    for d in range(1, M):
        j = lax.rem(me_t + d, M)
        send(hblk.at[j], hrow.at[pl.ds(me_t * T, T)], hid_s.at[d], hid_r.at[d], {"tok": j})
    hrow[pl.ds(pl.multiple_of(me_t * T, T), T), :] = hblk[me_t]

    for k in range(K):
        pltpu.make_async_copy(proj_hbm.at[k], w.at[k], w_sem.at[k]).wait()
        ctx[me_v, k * T:(k + 1) * T, :] = jnp.tanh(
            jnp.dot(hidden[...], w[k], preferred_element_type=F32)
        ).astype(BF16)
        piece = ctx.at[me_v, pl.ds(k * T, T)]
        for i in range(1, half):
            send(piece, piece, ctx_s.at[i, k], ctx_r.at[me_v, k],
                 {"voc": lax.rem(chip + i, half) * 2 + core})
        send(piece, piece, ctx_s.at[0, k], ctx_r.at[me_v, k], {"voc": partner})

    def add_logits(s, first=False):
        part = jnp.dot(ctx[s], vw[pl.ds(pl.multiple_of(s * E, E), E), :],
                       preferred_element_type=F32)
        logit[...] = part if first else logit[...] + part

    add_logits(me_v, True)
    for k in range(K):
        arrived(ctx.at[partner, pl.ds(k * T, T)], ctx_r.at[partner, k], ctx_s.at[0, k])
    add_logits(partner)

    tcol = column(targets[...].astype(F32), V)
    ids = (me_v * V + lax.broadcasted_iota(jnp.int32, (T, V), 1)).astype(F32)
    onehot = (tcol == ids).astype(F32)
    for d in range(1, N):
        arrived(mix_all.at[d], mix_r.at[d], mix_s.at[d])
    mixing = jnp.zeros((K, T), F32)
    for d in range(N):
        s = lax.rem(me_v - d + N, N)
        mixing = mixing + lax.dot_general(
            mix_all[d], hidden[:, pl.ds(pl.multiple_of(s * E, E), E)], NT,
            preferred_element_type=F32)
    exp_mix = jnp.exp(mixing)
    weights = exp_mix / jnp.sum(exp_mix, axis=0, keepdims=True)

    for i in range(1, half):
        s = lax.rem(chip - i + half, half) * 2 + core
        for k in range(K):
            piece = ctx.at[s, pl.ds(k * T, T)]
            arrived(piece, ctx_r.at[s, k], ctx_s.at[i, k])
            send(piece, piece, ctx_f.at[i, k], ctx_r.at[s, k], {"voc": partner})
        add_logits(s)
    for i in range(1, half):
        s = lax.rem(chip - i + half, half) * 2 + 1 - core
        for k in range(K):
            arrived(ctx.at[s, pl.ds(k * T, T)], ctx_r.at[s, k], ctx_s.at[i, k])
        add_logits(s)

    lane = lax.broadcasted_iota(jnp.int32, (T, 128), 1)
    table = jnp.zeros((T, 128), F32)
    for k in range(K):
        part = jnp.sum(logit[k * T:(k + 1) * T, :] * onehot, axis=1, keepdims=True)
        table = jnp.where(lane == k, part, table)
    tgt[0] = table.T[0:8, :]
    for d in range(1, N):
        send(tgt.at[0], tgt.at[d], tgt_s.at[d], tgt_r.at[d], {"voc": lax.rem(me_v + d, N)})
    for k in range(K):
        rows = slice(k * T, (k + 1) * T)
        logit[rows, :] = jnp.exp(logit[rows, :] - column(logz[k:k + 1, :], V)) - onehot
    for d in range(1, N):
        arrived(tgt.at[d], tgt_r.at[d], tgt_s.at[d])
    target = tgt[0]
    for d in range(1, N):
        target = target + tgt[d]
    likely = jnp.exp(target[0:K, :] - logz[...])
    joint = weights * likely
    posterior = joint / jnp.sum(joint, axis=0, keepdims=True)
    factor = loss[...] * posterior
    mgrad[...] = loss[...] * (weights - posterior)
    for k in range(K):
        rows = slice(k * T, (k + 1) * T)
        lg[rows, :] = (column(factor[k:k + 1, :], V) * logit[rows, :]).astype(BF16)

    def cg_part(s, k):
        return lax.dot_general(
            lg[k * T:(k + 1) * T, :], vw[pl.ds(pl.multiple_of(s * E, E), E), :], NT,
            preferred_element_type=F32)

    for i in list(range(1, half)) + [0]:
        s = lax.rem(chip + i, half) * 2
        for k in range(K):
            cgs[i, k] = cg_part(s + 1 - core, k).astype(BF16)
            send(cgs.at[i, k], cgr.at[i, k], cgp_s.at[i, k], cgp_r.at[i, k], {"voc": partner})
        for k in range(K):
            part = cg_part(s + core, k)
            if i == 0:
                own_cg[k] = part
            else:
                arrived(cgr.at[i, k], cgp_r.at[i, k], cgp_s.at[i, k])
                cgx[i, k] = (part + cgr[i, k].astype(F32)).astype(BF16)
                send(cgx.at[i, k], xr.at[i, k], cgx_s.at[i, k], cgx_r.at[i, k], {"voc": s + core})

    for s in range(N):
        vgb[s * E:(s + 1) * E, :] = lax.dot_general(
            ctx[s], lg[...], TN, preferred_element_type=F32).astype(BF16)
    for d in range(1, M):
        j = lax.rem(me_t + d, M)
        send(vgb.at[pl.ds(j * R, R)], vgr.at[d], vg_s.at[d], vg_r.at[d], {"tok": j})

    def rows_of(t):
        return pl.ds(pl.multiple_of(t * T, T), T)

    def relay(t, k, way, dev, pred=None):
        piece = pg.at[k, rows_of(t)]
        c = remote(piece, piece, ag_s.at[way, t, k], ag_r.at[t, k], {"tok": dev})
        if pred is None:
            c.start()
        else:
            pl.when(pred)(c.start)
        sends.append((pred, c))

    has_r = z + 1 < Z
    has_l = z >= 1
    for k in range(K):
        total = own_cg[k]
        arrived(cgr.at[0, k], cgp_r.at[0, k], cgp_s.at[0, k])
        total = total + cgr[0, k].astype(F32)
        for i in range(1, half):
            arrived(xr.at[i, k], cgx_r.at[i, k], cgx_s.at[i, k])
            total = total + xr[i, k].astype(F32)
        c = ctx[me_v, k * T:(k + 1) * T, :].astype(F32)
        pg[k, rows_of(me_t), :] = (total * (1.0 - c * c)).astype(BF16)
        if Z > 1:
            relay(me_t, k, 0, me_t + 2, has_r)
            relay(me_t, k, 1, me_t - 2, has_l)
        relay(me_t, k, 2, ypart)

    def hid_part(s):
        total = jnp.zeros((T, E), F32)
        for k in range(K):
            total = total + lax.dot_general(
                pg[k, rows_of(me_t), :], w[k, pl.ds(pl.multiple_of(s * E, E), E), :], NT,
                preferred_element_type=F32)
        return total

    for d in range(1, N):
        s = lax.rem(me_v + d, N)
        hss[d] = hid_part(s).astype(BF16)
        send(hss.at[d], hsr.at[d], hs_s.at[d], hs_r.at[d], {"voc": s})
    own_hs[...] = hid_part(me_v)

    for d in range(1, M):
        src = lax.rem(me_t - d + M, M)
        arrived(hrow.at[pl.ds(src * T, T)], hid_r.at[d], hid_s.at[d])

    def pair(zz, first=False):
        t = zz * 2 + 1 - y
        both = pl.ds(pl.multiple_of(zz * 2 * T, 2 * T), 2 * T)
        left = hrow[both, :].T
        for k in range(K):
            arrived(pg.at[k, rows_of(t)], ag_r.at[t, k], ag_s.at[2, t, k])
            part = jnp.dot(left, pg[k, both, :], preferred_element_type=F32)
            acc[k] = part if first else acc[k] + part

    def pairs(d):
        if d == 0:
            pair(z, True)
        else:
            pl.when(z >= d)(lambda: pair(z - d))
            pl.when(z + d < Z)(lambda: pair(z + d))

    for d in range(1, Z):
        from_l = z >= d
        from_r = z + d < Z
        for k in range(K):
            for there, t, way, dev, more in (
                (from_l, me_t - 2 * d, 0, me_t + 2, has_r),
                (from_r, me_t + 2 * d, 1, me_t - 2, has_l),
            ):
                def _(t=t, k=k):
                    arrived(pg.at[k, rows_of(t)], ag_r.at[t, k], ag_s.at[2, t, k])
                pl.when(there)(_)
                if d < Z - 1:
                    relay(t, k, way, dev, there & more)
                relay(t, k, 2, ypart, there)
        pairs(d - 1)

    vtot = vgb[rows_r(me_t, R), :].astype(F32)
    for d in range(1, M):
        arrived(vgr.at[d], vg_r.at[d], vg_s.at[d])
        vtot = vtot + vgr[d].astype(F32)
    out_vocab[...] = vtot.astype(BF16)
    htot = own_hs[...]
    for d in range(1, N):
        arrived(hsr.at[d], hs_r.at[d], hs_s.at[d])
        htot = htot + hsr[d].astype(F32)
    mixf = mix[...].astype(F32)
    for k in range(K):
        htot = htot + column(mgrad[k:k + 1, :], E) * mixf[k:k + 1, :]
    out_hidden[...] = htot.astype(BF16)

    pairs(Z - 1)
    for k in range(K):
        out_proj[k] = acc[k].astype(BF16)
    for pred, c in sends:
        if pred is None:
            c.wait_send()
        else:
            pl.when(pred)(c.wait_send)


def rows_r(t, R):
    return pl.ds(pl.multiple_of(t * R, R), R)


def body(M, N, hidden, mix_weight, comp_proj, vocab_weight, log_normalizer, targets, loss_grad):
    T, D = hidden.shape
    K, E = mix_weight.shape
    V = vocab_weight.shape[1]
    R = D // M
    half = N // 2
    w = jnp.transpose(comp_proj, (1, 0, 2))
    vm = pltpu.VMEM
    dma = pltpu.SemaphoreType.DMA
    scratch = [
        vm((K, D, E), BF16), vm((N, K * T, E), BF16), vm((N, K, E), BF16),
        vm((M, T, R), BF16), vm((M * T, R), BF16), vm((K * T, V), F32), vm((K * T, V), BF16),
        vm((N, 8, T), F32),
        vm((half, K, T, E), BF16), vm((half, K, T, E), BF16),
        vm((half, K, T, E), BF16), vm((half, K, T, E), BF16),
        vm((K, T, E), F32), vm((D, V), BF16), vm((M, R, V), BF16),
        vm((K, M * T, E), BF16), vm((N, T, E), BF16), vm((N, T, E), BF16),
        vm((T, E), F32), vm((K, R, E), F32), vm((K, T), F32),
        dma((K,)), dma((half, K)), dma((half, K)), dma((N, K)), dma((N,)), dma((N,)),
        dma((M,)), dma((M,)), dma((N,)), dma((N,)),
        dma((half, K)), dma((half, K)), dma((half, K)), dma((half, K)),
        dma((M,)), dma((M,)), dma((N,)), dma((N,)), dma((3, M, K)), dma((M, K)),
    ]
    spec = pl.BlockSpec(memory_space=pltpu.VMEM)
    hidden_grad, proj_grad, vocab_grad = pl.pallas_call(
        functools.partial(kernel, M, N),
        out_shape=(
            jax.ShapeDtypeStruct((T, E), BF16),
            jax.ShapeDtypeStruct((K, R, E), BF16),
            jax.ShapeDtypeStruct((R, V), BF16),
        ),
        in_specs=[spec, spec, pl.BlockSpec(memory_space=pl.ANY), spec, spec, spec, spec],
        out_specs=(spec, spec, spec),
        scratch_shapes=scratch,
        compiler_params=pltpu.CompilerParams(
            collective_id=0, has_side_effects=True, vmem_limit_bytes=56 * 1024 * 1024
        ),
    )(hidden, mix_weight, w, vocab_weight, log_normalizer, targets[None, :], loss_grad[None, :])
    return hidden_grad, jnp.transpose(proj_grad, (1, 0, 2)), vocab_grad


def solution(mesh):
    in_specs = (
        P("tok", None),
        P(None, "voc"),
        P(None, None, "voc"),
        P(None, "voc"),
        P(None, "tok"),
        P("tok"),
        P("tok"),
    )
    out_specs = (P("tok", "voc"), P("tok", None, "voc"), P("tok", "voc"))
    return jax.shard_map(
        functools.partial(body, mesh.shape["tok"], mesh.shape["voc"]),
        mesh=mesh, in_specs=in_specs, out_specs=out_specs, check_vma=False,
    )
```

```python
import functools

import jax
import jax.numpy as jnp
from jax import lax
from jax.experimental import pallas as pl
from jax.experimental.pallas import tpu as pltpu
from jax.sharding import PartitionSpec as P

MESH = pl.DeviceIdType.MESH
F32 = jnp.float32
BF16 = jnp.bfloat16
NT = (((1,), (1,)), ((), ()))
TN = (((0,), (0,)), ((), ()))


def column(row, lanes):
    wide = jnp.broadcast_to(row, (128, row.shape[1])).T
    return jnp.concatenate([wide] * (lanes // 128), axis=1)


def kernel(
    M, N,
    hidden, mix, proj_hbm, vw, logz, targets, loss,
    out_hidden, out_proj, out_vocab,
    w, ctx, mix_all, hblk, hrow, htr, logit, lg, tgt,
    cgs, cgr, cgx, xr, own_cg, vgb, vgy, vsum, vout, vin, pg, hss, hsr, own_hs, acc, psend, precv, mgrad,
    w_sem, ctx_s, ctx_f, ctx_r, mix_s, mix_r, hid_s, hid_r, tgt_s, tgt_r,
    cgp_s, cgp_r, cgx_s, cgx_r, vy_s, vy_r, vz_s, vz_r, hs_s, hs_r, ag_s, ag_r, pp_s, pp_r,
):
    K, D, E = w.shape
    T = hidden.shape[0]
    V = vw.shape[1]
    R = D // M
    half = N // 2
    Z = M // 2
    me_t = lax.axis_index("tok")
    me_v = lax.axis_index("voc")
    chip = me_v // 2
    core = me_v % 2
    partner = me_v + 1 - 2 * core
    z = me_t // 2
    y = me_t % 2
    ypart = me_t + 1 - 2 * y
    sends = []

    def remote(src, dst, ss, rs, dev):
        return pltpu.make_async_remote_copy(
            src_ref=src, dst_ref=dst, send_sem=ss, recv_sem=rs,
            device_id=dev, device_id_type=MESH,
        )

    def send(src, dst, ss, rs, dev):
        c = remote(src, dst, ss, rs, dev)
        c.start()
        sends.append((None, c))

    def arrived(ref, rs, ss):
        remote(ref, ref, ss, rs, {"voc": partner}).wait_recv()

    for k in range(K):
        pltpu.make_async_copy(proj_hbm.at[k], w.at[k], w_sem.at[k]).start()
    for j in range(M):
        hblk[j // 2, j % 2] = hidden[:, j * R:(j + 1) * R]

    bar = pltpu.get_barrier_semaphore()
    for d in range(1, M):
        pl.semaphore_signal(bar, inc=1, device_id={"tok": lax.rem(me_t + d, M)}, device_id_type=MESH)
    for d in range(1, N):
        pl.semaphore_signal(bar, inc=1, device_id={"voc": lax.rem(me_v + d, N)}, device_id_type=MESH)
    pl.semaphore_wait(bar, M + N - 2)

    for d in range(1, N):
        send(mix, mix_all.at[d], mix_s.at[d], mix_r.at[d], {"voc": lax.rem(me_v + d, N)})
    mix_all[0] = mix[...]
    for d in range(1, Z):
        zz = lax.rem(z + d, Z)
        send(hblk.at[zz], hrow.at[:, pl.ds(z * T, T)], hid_s.at[d], hid_r.at[d],
             {"tok": zz * 2 + y})
    hrow[:, rows_of(z, T), :] = hblk[z]

    for k in range(K):
        pltpu.make_async_copy(proj_hbm.at[k], w.at[k], w_sem.at[k]).wait()
        ctx[me_v, k * T:(k + 1) * T, :] = jnp.tanh(
            jnp.dot(hidden[...], w[k], preferred_element_type=F32)
        ).astype(BF16)
        piece = ctx.at[me_v, pl.ds(k * T, T)]
        for i in range(1, half):
            send(piece, piece, ctx_s.at[i, k], ctx_r.at[me_v, k],
                 {"voc": lax.rem(chip + i, half) * 2 + core})
        send(piece, piece, ctx_s.at[0, k], ctx_r.at[me_v, k], {"voc": partner})

    def add_logits(s, first=False):
        part = jnp.dot(ctx[s], vw[pl.ds(pl.multiple_of(s * E, E), E), :],
                       preferred_element_type=F32)
        logit[...] = part if first else logit[...] + part

    add_logits(me_v, True)
    for k in range(K):
        arrived(ctx.at[partner, pl.ds(k * T, T)], ctx_r.at[partner, k], ctx_s.at[0, k])
    add_logits(partner)

    tcol = column(targets[...].astype(F32), V)
    ids = (me_v * V + lax.broadcasted_iota(jnp.int32, (T, V), 1)).astype(F32)
    onehot = (tcol == ids).astype(F32)
    for d in range(1, N):
        arrived(mix_all.at[d], mix_r.at[d], mix_s.at[d])
    mixing = jnp.zeros((K, T), F32)
    for d in range(N):
        s = lax.rem(me_v - d + N, N)
        mixing = mixing + lax.dot_general(
            mix_all[d], hidden[:, pl.ds(pl.multiple_of(s * E, E), E)], NT,
            preferred_element_type=F32)
    exp_mix = jnp.exp(mixing)
    weights = exp_mix / jnp.sum(exp_mix, axis=0, keepdims=True)

    for i in range(1, half):
        s = lax.rem(chip - i + half, half) * 2 + core
        for k in range(K):
            piece = ctx.at[s, pl.ds(k * T, T)]
            arrived(piece, ctx_r.at[s, k], ctx_s.at[i, k])
            send(piece, piece, ctx_f.at[i, k], ctx_r.at[s, k], {"voc": partner})
        add_logits(s)
    for i in range(1, half):
        s = lax.rem(chip - i + half, half) * 2 + 1 - core
        for k in range(K):
            arrived(ctx.at[s, pl.ds(k * T, T)], ctx_r.at[s, k], ctx_s.at[i, k])
        add_logits(s)

    lane = lax.broadcasted_iota(jnp.int32, (T, 128), 1)
    table = jnp.zeros((T, 128), F32)
    for k in range(K):
        part = jnp.sum(logit[k * T:(k + 1) * T, :] * onehot, axis=1, keepdims=True)
        table = jnp.where(lane == k, part, table)
    tgt[0] = table.T[0:8, :]
    for d in range(1, N):
        send(tgt.at[0], tgt.at[d], tgt_s.at[d], tgt_r.at[d], {"voc": lax.rem(me_v + d, N)})
    for k in range(K):
        rows = slice(k * T, (k + 1) * T)
        logit[rows, :] = jnp.exp(logit[rows, :] - column(logz[k:k + 1, :], V)) - onehot
    for d in range(1, N):
        arrived(tgt.at[d], tgt_r.at[d], tgt_s.at[d])
    target = tgt[0]
    for d in range(1, N):
        target = target + tgt[d]
    likely = jnp.exp(target[0:K, :] - logz[...])
    joint = weights * likely
    posterior = joint / jnp.sum(joint, axis=0, keepdims=True)
    factor = loss[...] * posterior
    mgrad[...] = loss[...] * (weights - posterior)
    for k in range(K):
        rows = slice(k * T, (k + 1) * T)
        lg[rows, :] = (column(factor[k:k + 1, :], V) * logit[rows, :]).astype(BF16)

    def cg_part(s, k):
        return lax.dot_general(
            lg[k * T:(k + 1) * T, :], vw[pl.ds(pl.multiple_of(s * E, E), E), :], NT,
            preferred_element_type=F32)

    for i in list(range(1, half)) + [0]:
        s = lax.rem(chip + i, half) * 2
        for k in range(K):
            cgs[i, k] = cg_part(s + 1 - core, k).astype(BF16)
            send(cgs.at[i, k], cgr.at[i, k], cgp_s.at[i, k], cgp_r.at[i, k], {"voc": partner})
        for k in range(K):
            part = cg_part(s + core, k)
            if i == 0:
                own_cg[k] = part
            else:
                arrived(cgr.at[i, k], cgp_r.at[i, k], cgp_s.at[i, k])
                cgx[i, k] = (part + cgr[i, k].astype(F32)).astype(BF16)
                send(cgx.at[i, k], xr.at[i, k], cgx_s.at[i, k], cgx_r.at[i, k], {"voc": s + core})

    for s in range(N):
        vgb[s * E:(s + 1) * E, :] = lax.dot_general(
            ctx[s], lg[...], TN, preferred_element_type=F32).astype(BF16)
    for zz in range(Z):
        send(vgb.at[pl.ds((zz * 2 + 1 - y) * R, R)], vgy.at[zz], vy_s.at[zz], vy_r.at[zz],
             {"tok": ypart})

    def relay(t, k, way, pred):
        piece = pg.at[k, rows_of(t, T)]
        c = remote(piece, piece, ag_s.at[way, t, k], ag_r.at[t, k],
                   {"tok": me_t + 2 - 4 * way})
        pl.when(pred)(c.start)
        sends.append((pred, c))

    has_r = z + 1 < Z
    has_l = z >= 1
    for k in range(K):
        total = own_cg[k]
        arrived(cgr.at[0, k], cgp_r.at[0, k], cgp_s.at[0, k])
        total = total + cgr[0, k].astype(F32)
        for i in range(1, half):
            arrived(xr.at[i, k], cgx_r.at[i, k], cgx_s.at[i, k])
            total = total + xr[i, k].astype(F32)
        c = ctx[me_v, k * T:(k + 1) * T, :].astype(F32)
        pg[k, rows_of(z, T), :] = (total * (1.0 - c * c)).astype(BF16)
        if Z > 1:
            relay(z, k, 0, has_r)
            relay(z, k, 1, has_l)

    def hid_part(s):
        total = jnp.zeros((T, E), F32)
        for k in range(K):
            total = total + lax.dot_general(
                pg[k, rows_of(z, T), :], w[k, pl.ds(pl.multiple_of(s * E, E), E), :], NT,
                preferred_element_type=F32)
        return total

    for d in range(1, N):
        s = lax.rem(me_v + d, N)
        hss[d] = hid_part(s).astype(BF16)
        send(hss.at[d], hsr.at[d], hs_s.at[d], hs_r.at[d], {"voc": s})
    own_hs[...] = hid_part(me_v)

    for zz in range(Z):
        arrived(vgy.at[zz], vy_r.at[zz], vy_s.at[zz])
        vsum[zz] = vgb[rows_of(zz * 2 + y, R), :].astype(F32) + vgy[zz].astype(F32)

    def hop(h):
        for way, at, ends in ((0, h, range(h + 1, Z)), (1, Z - 1 - h, range(Z - 1 - h))):
            copies = [
                remote(vout.at[way, e], vin.at[way, e], vz_s.at[way, e], vz_r.at[way, e],
                       {"tok": me_t + 2 - 4 * way})
                for e in ends
            ]

            @pl.when(z == at)
            def _(way=way, ends=ends, copies=copies):
                for e, c in zip(ends, copies):
                    part = vsum[e]
                    if h > 0:
                        arrived(vin.at[way, e], vz_r.at[way, e], vz_s.at[way, e])
                        part = part + vin[way, e].astype(F32)
                    vout[way, e] = part.astype(BF16)
                    c.start()
            for c in copies:
                sends.append((z == at, c))

    for d in range(1, Z):
        src = lax.rem(z - d + Z, Z)
        arrived(hrow.at[:, pl.ds(src * T, T)], hid_r.at[d], hid_s.at[d])
    for b in range(2):
        htr[b] = hrow[b].T

    per = pl.cdiv(max(Z - 1, 1), K)
    for k in range(K):
        for h in range(k * per, min((k + 1) * per, Z - 1)):
            hop(h)
        for d in range(1, Z):
            for there, t, way, more in (
                (z >= d, z - d, 0, has_r), (z + d < Z, z + d, 1, has_l),
            ):
                def _(t=t, k=k):
                    arrived(pg.at[k, rows_of(t, T)], ag_r.at[t, k], ag_s.at[0, t, k])
                pl.when(there)(_)
                if d < Z - 1:
                    relay(t, k, way, there & more)
        psend[k] = jnp.dot(htr[1 - y], pg[k], preferred_element_type=F32).astype(BF16)
        send(psend.at[k], precv.at[k], pp_s.at[k], pp_r.at[k], {"tok": ypart})
        acc[k] = jnp.dot(htr[y], pg[k], preferred_element_type=F32)

    acc_v = vsum.at[z]
    for way, pred in ((0, has_l), (1, has_r)):
        @pl.when(pred)
        def _(way=way):
            arrived(vin.at[way, z], vz_r.at[way, z], vz_s.at[way, z])
            acc_v[...] += vin[way, z].astype(F32)
    out_vocab[...] = acc_v[...].astype(BF16)
    htot = own_hs[...]
    for d in range(1, N):
        arrived(hsr.at[d], hs_r.at[d], hs_s.at[d])
        htot = htot + hsr[d].astype(F32)
    mixf = mix[...].astype(F32)
    for k in range(K):
        htot = htot + column(mgrad[k:k + 1, :], E) * mixf[k:k + 1, :]
    out_hidden[...] = htot.astype(BF16)

    for k in range(K):
        arrived(precv.at[k], pp_r.at[k], pp_s.at[k])
        out_proj[k] = (acc[k] + precv[k].astype(F32)).astype(BF16)
    for pred, c in sends:
        if pred is None:
            c.wait_send()
        else:
            pl.when(pred)(c.wait_send)


def rows_of(block, size):
    return pl.ds(pl.multiple_of(block * size, size), size)


def body(M, N, hidden, mix_weight, comp_proj, vocab_weight, log_normalizer, targets, loss_grad):
    T, D = hidden.shape
    K, E = mix_weight.shape
    V = vocab_weight.shape[1]
    R = D // M
    half = N // 2
    Z = M // 2
    w = jnp.transpose(comp_proj, (1, 0, 2))
    vm = pltpu.VMEM
    dma = pltpu.SemaphoreType.DMA
    scratch = [
        vm((K, D, E), BF16), vm((N, K * T, E), BF16), vm((N, K, E), BF16),
        vm((Z, 2, T, R), BF16), vm((2, Z * T, R), BF16), vm((2, R, Z * T), BF16), vm((K * T, V), F32), vm((K * T, V), BF16),
        vm((N, 8, T), F32),
        vm((half, K, T, E), BF16), vm((half, K, T, E), BF16),
        vm((half, K, T, E), BF16), vm((half, K, T, E), BF16),
        vm((K, T, E), F32), vm((D, V), BF16), vm((Z, R, V), BF16),
        vm((Z, R, V), F32), vm((2, Z, R, V), BF16), vm((2, Z, R, V), BF16),
        vm((K, Z * T, E), BF16), vm((N, T, E), BF16), vm((N, T, E), BF16),
        vm((T, E), F32), vm((K, R, E), F32), vm((K, R, E), BF16), vm((K, R, E), BF16),
        vm((K, T), F32),
        dma((K,)), dma((half, K)), dma((half, K)), dma((N, K)), dma((N,)), dma((N,)),
        dma((Z,)), dma((Z,)), dma((N,)), dma((N,)),
        dma((half, K)), dma((half, K)), dma((half, K)), dma((half, K)),
        dma((Z,)), dma((Z,)), dma((2, Z)), dma((2, Z)), dma((N,)), dma((N,)),
        dma((2, Z, K)), dma((Z, K)), dma((K,)), dma((K,)),
    ]
    spec = pl.BlockSpec(memory_space=pltpu.VMEM)
    hidden_grad, proj_grad, vocab_grad = pl.pallas_call(
        functools.partial(kernel, M, N),
        out_shape=(
            jax.ShapeDtypeStruct((T, E), BF16),
            jax.ShapeDtypeStruct((K, R, E), BF16),
            jax.ShapeDtypeStruct((R, V), BF16),
        ),
        in_specs=[spec, spec, pl.BlockSpec(memory_space=pltpu.MemorySpace.HBM)] + [spec] * 4,
        out_specs=(spec, spec, spec),
        scratch_shapes=scratch,
        compiler_params=pltpu.CompilerParams(
            collective_id=0, has_side_effects=True, vmem_limit_bytes=48 * 1024 * 1024
        ),
    )(hidden, mix_weight, w, vocab_weight, log_normalizer, targets[None, :], loss_grad[None, :])
    return hidden_grad, jnp.transpose(proj_grad, (1, 0, 2)), vocab_grad


def solution(mesh):
    in_specs = (
        P("tok", None),
        P(None, "voc"),
        P(None, None, "voc"),
        P(None, "voc"),
        P(None, "tok"),
        P("tok"),
        P("tok"),
    )
    out_specs = (P("tok", "voc"), P("tok", None, "voc"), P("tok", "voc"))
    return jax.shard_map(
        functools.partial(body, mesh.shape["tok"], mesh.shape["voc"]),
        mesh=mesh, in_specs=in_specs, out_specs=out_specs, check_vma=False,
    )
```

```python
import functools

import jax
import jax.numpy as jnp
from jax import lax
from jax.experimental import pallas as pl
from jax.experimental.pallas import tpu as pltpu
from jax.sharding import PartitionSpec as P

MESH = pl.DeviceIdType.MESH
F32 = jnp.float32
BF16 = jnp.bfloat16
NT = (((1,), (1,)), ((), ()))
TN = (((0,), (0,)), ((), ()))


def column(row, lanes):
    wide = jnp.broadcast_to(row, (128, row.shape[1])).T
    return jnp.concatenate([wide] * (lanes // 128), axis=1)


def kernel(
    M, N,
    hidden, mix, proj_hbm, vw, logz, targets, loss,
    out_hidden, out_proj, out_vocab,
    w, ctx, mix_all, hblk, hrow, htr, logit, lg, tgt,
    cgs, cgr, cgx, xr, own_cg, vgb, vgy, vsum, vout, vin, pg, hss, hsr, own_hs, acc, psend, precv, mgrad,
    w_sem, ctx_s, ctx_f, ctx_r, mix_s, mix_r, hid_s, hid_r, tgt_s, tgt_r,
    cgp_s, cgp_r, cgx_s, cgx_r, vy_s, vy_r, vz_s, vz_r, hs_s, hs_r, ag_s, ag_r, pp_s, pp_r,
):
    K, D, E = w.shape
    T = hidden.shape[0]
    V = vw.shape[1]
    R = D // M
    half = N // 2
    Z = M // 2
    H = 2
    TH = T // H
    Q = K * TH // T
    me_t = lax.axis_index("tok")
    me_v = lax.axis_index("voc")
    chip = me_v // 2
    core = me_v % 2
    partner = me_v + 1 - 2 * core
    z = me_t // 2
    y = me_t % 2
    ypart = me_t + 1 - 2 * y
    sends = []

    def remote(src, dst, ss, rs, dev):
        return pltpu.make_async_remote_copy(
            src_ref=src, dst_ref=dst, send_sem=ss, recv_sem=rs,
            device_id=dev, device_id_type=MESH,
        )

    def send(src, dst, ss, rs, dev):
        c = remote(src, dst, ss, rs, dev)
        c.start()
        sends.append((None, c))

    def arrived(ref, rs, ss):
        remote(ref, ref, ss, rs, {"voc": partner}).wait_recv()

    for k in range(K):
        pltpu.make_async_copy(proj_hbm.at[k], w.at[k], w_sem.at[k]).start()
    for j in range(M):
        hblk[j // 2, j % 2] = hidden[:, j * R:(j + 1) * R]

    bar = pltpu.get_barrier_semaphore()
    for d in range(1, M):
        pl.semaphore_signal(bar, inc=1, device_id={"tok": lax.rem(me_t + d, M)}, device_id_type=MESH)
    for d in range(1, N):
        pl.semaphore_signal(bar, inc=1, device_id={"voc": lax.rem(me_v + d, N)}, device_id_type=MESH)
    pl.semaphore_wait(bar, M + N - 2)

    for d in range(1, N):
        send(mix, mix_all.at[d], mix_s.at[d], mix_r.at[d], {"voc": lax.rem(me_v + d, N)})
    mix_all[0] = mix[...]
    for d in range(1, Z):
        zz = lax.rem(z + d, Z)
        send(hblk.at[zz], hrow.at[:, pl.ds(z * T, T)], hid_s.at[d], hid_r.at[d],
             {"tok": zz * 2 + y})
    hrow[:, rows_of(z, T), :] = hblk[z]

    def send_context(h, k):
        piece = ctx.at[me_v, h, pl.ds(k * TH, TH)]
        for i in range(1, half):
            send(piece, piece, ctx_s.at[i, h, k], ctx_r.at[me_v, h, k],
                 {"voc": lax.rem(chip + i, half) * 2 + core})
        send(piece, piece, ctx_s.at[0, h, k], ctx_r.at[me_v, h, k], {"voc": partner})

    for k in range(K):
        pltpu.make_async_copy(proj_hbm.at[k], w.at[k], w_sem.at[k]).wait()
        own = jnp.tanh(
            jnp.dot(hidden[...], w[k], preferred_element_type=F32)
        ).astype(BF16)
        for h in range(H):
            ctx[me_v, h, k * TH:(k + 1) * TH, :] = own[h * TH:(h + 1) * TH]
        send_context(0, k)
    for h in range(1, H):
        for k in range(K):
            send_context(h, k)

    def add_logits(s, h, first=False):
        part = jnp.dot(ctx[s, h], vw[pl.ds(pl.multiple_of(s * E, E), E), :],
                       preferred_element_type=F32)
        logit[h] = part if first else logit[h] + part

    def near_logits(h):
        add_logits(me_v, h, True)
        for k in range(K):
            arrived(ctx.at[partner, h, pl.ds(k * TH, TH)], ctx_r.at[partner, h, k], ctx_s.at[0, h, k])
        add_logits(partner, h)

    near_logits(0)

    tcol = column(targets[...].astype(F32), V)
    ids = (me_v * V + lax.broadcasted_iota(jnp.int32, (T, V), 1)).astype(F32)
    onehot = (tcol == ids).astype(F32)
    for d in range(1, N):
        arrived(mix_all.at[d], mix_r.at[d], mix_s.at[d])
    mixing = jnp.zeros((K, T), F32)
    for d in range(N):
        s = lax.rem(me_v - d + N, N)
        mixing = mixing + lax.dot_general(
            mix_all[d], hidden[:, pl.ds(pl.multiple_of(s * E, E), E)], NT,
            preferred_element_type=F32)
    exp_mix = jnp.exp(mixing)
    weights = exp_mix / jnp.sum(exp_mix, axis=0, keepdims=True)

    lane = lax.broadcasted_iota(jnp.int32, (TH, 128), 1)
    norm = [column(logz[k:k + 1, :], V) for k in range(K)]

    def cut(k):
        return slice(k * TH, (k + 1) * TH)

    def far_logits(h):
        for i in range(1, half):
            s = lax.rem(chip - i + half, half) * 2 + core
            for k in range(K):
                piece = ctx.at[s, h, pl.ds(k * TH, TH)]
                arrived(piece, ctx_r.at[s, h, k], ctx_s.at[i, h, k])
                send(piece, piece, ctx_f.at[i, h, k], ctx_r.at[s, h, k], {"voc": partner})
            add_logits(s, h)
        for i in range(1, half):
            s = lax.rem(chip - i + half, half) * 2 + 1 - core
            for k in range(K):
                arrived(ctx.at[s, h, pl.ds(k * TH, TH)], ctx_r.at[s, h, k], ctx_s.at[i, h, k])
            add_logits(s, h)
        table = jnp.zeros((TH, 128), F32)
        for k in range(K):
            part = jnp.sum(logit[h, cut(k), :] * onehot[cut(h)], axis=1, keepdims=True)
            table = jnp.where(lane == k, part, table)
        zero = jnp.zeros((TH, 128), F32)
        tgt[h, 0] = jnp.concatenate([table if g == h else zero for g in range(H)], axis=0).T[0:8, :]
        for d in range(1, N):
            send(tgt.at[h, 0], tgt.at[h, d], tgt_s.at[h, d], tgt_r.at[h, d],
                 {"voc": lax.rem(me_v + d, N)})
        for k in range(K):
            logit[h, cut(k), :] = jnp.exp(logit[h, cut(k), :] - norm[k][cut(h)]) - onehot[cut(h)]

    def cg_part(s, h, q):
        return lax.dot_general(
            lg[h, q * T:(q + 1) * T, :], vw[pl.ds(pl.multiple_of(s * E, E), E), :], NT,
            preferred_element_type=F32)

    def gradients(h):
        for d in range(1, N):
            arrived(tgt.at[h, d], tgt_r.at[h, d], tgt_s.at[h, d])
        target = tgt[h, 0]
        for d in range(1, N):
            target = target + tgt[h, d]
        likely = jnp.exp(target[0:K, :] - logz[...])
        joint = weights * likely
        posterior = joint / jnp.sum(joint, axis=0, keepdims=True)
        factor = loss[...] * posterior
        slope = loss[...] * (weights - posterior)
        token = lax.broadcasted_iota(jnp.int32, (K, T), 1)
        mgrad[...] = slope if h == 0 else jnp.where(token >= h * TH, slope, mgrad[...])
        for k in range(K):
            lg[h, cut(k), :] = (
                column(factor[k:k + 1, :], V)[cut(h)] * logit[h, cut(k), :]).astype(BF16)
        for i in list(range(1, half)) + [0]:
            s = lax.rem(chip + i, half) * 2
            for q in range(Q):
                cgs[i, h, q] = cg_part(s + 1 - core, h, q).astype(BF16)
                send(cgs.at[i, h, q], cgr.at[i, h, q], cgp_s.at[i, h, q], cgp_r.at[i, h, q],
                     {"voc": partner})
            for q in range(Q):
                part = cg_part(s + core, h, q)
                if i == 0:
                    own_cg[h, q] = part
                else:
                    arrived(cgr.at[i, h, q], cgp_r.at[i, h, q], cgp_s.at[i, h, q])
                    cgx[i, h, q] = (part + cgr[i, h, q].astype(F32)).astype(BF16)
                    send(cgx.at[i, h, q], xr.at[i, h, q], cgx_s.at[i, h, q], cgx_r.at[i, h, q],
                         {"voc": s + core})

    far_logits(0)
    near_logits(1)
    gradients(0)
    far_logits(1)
    gradients(1)

    for s in range(N):
        vgb[s * E:(s + 1) * E, :] = sum(
            lax.dot_general(ctx[s, h], lg[h], TN, preferred_element_type=F32) for h in range(H)
        ).astype(BF16)
    for zz in range(Z):
        send(vgb.at[pl.ds((zz * 2 + 1 - y) * R, R)], vgy.at[zz], vy_s.at[zz], vy_r.at[zz],
             {"tok": ypart})

    pieces = [(k, 0, E) for k in range(K)]
    if E % 256 == 0:
        pieces[-1:] = [(K - 1, 0, E // 2), (K - 1, E // 2, E // 2)]

    def relay(t, p, way, pred, h=None):
        k, lo, wide = pieces[p]
        rows = rows_of(t, T) if h is None else rows_of(t * H + h, TH)
        piece = pg.at[k, rows, pl.ds(lo, wide)]
        c = remote(piece, piece, ag_s.at[way, t, p, 0 if h is None else h], ag_r.at[t, p],
                   {"tok": me_t + 2 - 4 * way})
        pl.when(pred)(c.start)
        sends.append((pred, c))

    has_r = z + 1 < Z
    has_l = z >= 1
    for h in range(H):
        for q in range(Q):
            arrived(cgr.at[0, h, q], cgp_r.at[0, h, q], cgp_s.at[0, h, q])
            total = own_cg[h, q] + cgr[0, h, q].astype(F32)
            for i in range(1, half):
                arrived(xr.at[i, h, q], cgx_r.at[i, h, q], cgx_s.at[i, h, q])
                total = total + xr[i, h, q].astype(F32)
            c = ctx[me_v, h, q * T:(q + 1) * T, :].astype(F32)
            grad = (total * (1.0 - c * c)).astype(BF16)
            for g in range(H):
                pg[q * H + g, rows_of(z * H + h, TH), :] = grad[g * TH:(g + 1) * TH]
            if Z > 1:
                for p, (k, lo, wide) in enumerate(pieces):
                    if k // H == q:
                        relay(z, p, 0, has_r, h)
                        relay(z, p, 1, has_l, h)

    def hid_part(s):
        total = jnp.zeros((T, E), F32)
        for k in range(K):
            total = total + lax.dot_general(
                pg[k, rows_of(z, T), :], w[k, pl.ds(pl.multiple_of(s * E, E), E), :], NT,
                preferred_element_type=F32)
        return total

    for d in range(1, N):
        s = lax.rem(me_v + d, N)
        hss[d] = hid_part(s).astype(BF16)
        send(hss.at[d], hsr.at[d], hs_s.at[d], hs_r.at[d], {"voc": s})
    own_hs[...] = hid_part(me_v)

    for zz in range(Z):
        arrived(vgy.at[zz], vy_r.at[zz], vy_s.at[zz])
        vsum[zz] = vgb[rows_of(zz * 2 + y, R), :].astype(F32) + vgy[zz].astype(F32)

    def hop(h):
        for way, at, ends in ((0, h, range(h + 1, Z)), (1, Z - 1 - h, range(Z - 1 - h))):
            copies = [
                remote(vout.at[way, e], vin.at[way, e], vz_s.at[way, e], vz_r.at[way, e],
                       {"tok": me_t + 2 - 4 * way})
                for e in ends
            ]

            @pl.when(z == at)
            def _(way=way, ends=ends, copies=copies):
                for e, c in zip(ends, copies):
                    part = vsum[e]
                    if h > 0:
                        arrived(vin.at[way, e], vz_r.at[way, e], vz_s.at[way, e])
                        part = part + vin[way, e].astype(F32)
                    vout[way, e] = part.astype(BF16)
                    c.start()
            for c in copies:
                sends.append((z == at, c))

    for d in range(1, Z):
        src = lax.rem(z - d + Z, Z)
        arrived(hrow.at[:, pl.ds(src * T, T)], hid_r.at[d], hid_s.at[d])
    for b in range(2):
        htr[b] = hrow[b].T

    per = pl.cdiv(max(Z - 1, 1), K)
    for p, (k, lo, wide) in enumerate(pieces):
        lanes = slice(lo, lo + wide)
        for h in range(p * per, min((p + 1) * per, Z - 1)):
            hop(h)
        for d in range(1, Z):
            for there, t, way, more in (
                (z >= d, z - d, 0, has_r), (z + d < Z, z + d, 1, has_l),
            ):
                def _(t=t):
                    arrived(pg.at[k, rows_of(t, T), pl.ds(lo, wide)], ag_r.at[t, p], ag_s.at[0, t, p, 0])
                pl.when(there)(_)
                if d < Z - 1:
                    relay(t, p, way, there & more)
        psend[k, :, lanes] = jnp.dot(
            htr[1 - y], pg[k, :, lanes], preferred_element_type=F32).astype(BF16)
        send(psend.at[k, :, pl.ds(lo, wide)], precv.at[k, :, pl.ds(lo, wide)],
             pp_s.at[p], pp_r.at[p], {"tok": ypart})
        acc[k, :, lanes] = jnp.dot(htr[y], pg[k, :, lanes], preferred_element_type=F32)

    acc_v = vsum.at[z]
    for way, pred in ((0, has_l), (1, has_r)):
        @pl.when(pred)
        def _(way=way):
            arrived(vin.at[way, z], vz_r.at[way, z], vz_s.at[way, z])
            acc_v[...] += vin[way, z].astype(F32)
    out_vocab[...] = acc_v[...].astype(BF16)
    htot = own_hs[...]
    for d in range(1, N):
        arrived(hsr.at[d], hs_r.at[d], hs_s.at[d])
        htot = htot + hsr[d].astype(F32)
    mixf = mix[...].astype(F32)
    for k in range(K):
        htot = htot + column(mgrad[k:k + 1, :], E) * mixf[k:k + 1, :]
    out_hidden[...] = htot.astype(BF16)

    for p, (k, lo, wide) in enumerate(pieces):
        lanes = slice(lo, lo + wide)
        arrived(precv.at[k, :, pl.ds(lo, wide)], pp_r.at[p], pp_s.at[p])
        out_proj[k, :, lanes] = (acc[k, :, lanes] + precv[k, :, lanes].astype(F32)).astype(BF16)
    for pred, c in sends:
        if pred is None:
            c.wait_send()
        else:
            pl.when(pred)(c.wait_send)


def rows_of(block, size):
    return pl.ds(pl.multiple_of(block * size, size), size)


def body(M, N, hidden, mix_weight, comp_proj, vocab_weight, log_normalizer, targets, loss_grad):
    T, D = hidden.shape
    K, E = mix_weight.shape
    V = vocab_weight.shape[1]
    R = D // M
    half = N // 2
    Z = M // 2
    H = 2
    TH = T // H
    Q = K * TH // T
    w = jnp.transpose(comp_proj, (1, 0, 2))
    vm = pltpu.VMEM
    dma = pltpu.SemaphoreType.DMA
    scratch = [
        vm((K, D, E), BF16), vm((N, H, K * TH, E), BF16), vm((N, K, E), BF16),
        vm((Z, 2, T, R), BF16), vm((2, Z * T, R), BF16), vm((2, R, Z * T), BF16), vm((H, K * TH, V), F32), vm((H, K * TH, V), BF16),
        vm((H, N, 8, T), F32),
        vm((half, H, Q, T, E), BF16), vm((half, H, Q, T, E), BF16),
        vm((half, H, Q, T, E), BF16), vm((half, H, Q, T, E), BF16),
        vm((H, Q, T, E), F32), vm((D, V), BF16), vm((Z, R, V), BF16),
        vm((Z, R, V), F32), vm((2, Z, R, V), BF16), vm((2, Z, R, V), BF16),
        vm((K, Z * T, E), BF16), vm((N, T, E), BF16), vm((N, T, E), BF16),
        vm((T, E), F32), vm((K, R, E), F32), vm((K, R, E), BF16), vm((K, R, E), BF16),
        vm((K, T), F32),
        dma((K,)), dma((half, H, K)), dma((half, H, K)), dma((N, H, K)), dma((N,)), dma((N,)),
        dma((Z,)), dma((Z,)), dma((H, N)), dma((H, N)),
        dma((half, H, Q)), dma((half, H, Q)), dma((half, H, Q)), dma((half, H, Q)),
        dma((Z,)), dma((Z,)), dma((2, Z)), dma((2, Z)), dma((N,)), dma((N,)),
        dma((2, Z, K + 1, H)), dma((Z, K + 1)), dma((K + 1,)), dma((K + 1,)),
    ]
    spec = pl.BlockSpec(memory_space=pltpu.VMEM)
    hidden_grad, proj_grad, vocab_grad = pl.pallas_call(
        functools.partial(kernel, M, N),
        out_shape=(
            jax.ShapeDtypeStruct((T, E), BF16),
            jax.ShapeDtypeStruct((K, R, E), BF16),
            jax.ShapeDtypeStruct((R, V), BF16),
        ),
        in_specs=[spec, spec, pl.BlockSpec(memory_space=pltpu.MemorySpace.HBM)] + [spec] * 4,
        out_specs=(spec, spec, spec),
        scratch_shapes=scratch,
        compiler_params=pltpu.CompilerParams(
            collective_id=0, has_side_effects=True, vmem_limit_bytes=48 * 1024 * 1024
        ),
    )(hidden, mix_weight, w, vocab_weight, log_normalizer, targets[None, :], loss_grad[None, :])
    return hidden_grad, jnp.transpose(proj_grad, (1, 0, 2)), vocab_grad


def solution(mesh):
    in_specs = (
        P("tok", None),
        P(None, "voc"),
        P(None, None, "voc"),
        P(None, "voc"),
        P(None, "tok"),
        P("tok"),
        P("tok"),
    )
    out_specs = (P("tok", "voc"), P("tok", None, "voc"), P("tok", "voc"))
    return jax.shard_map(
        functools.partial(body, mesh.shape["tok"], mesh.shape["voc"]),
        mesh=mesh, in_specs=in_specs, out_specs=out_specs, check_vma=False,
    )
```

```python
import functools

import jax
import jax.numpy as jnp
from jax import lax
from jax.experimental import pallas as pl
from jax.experimental.pallas import tpu as pltpu
from jax.sharding import PartitionSpec as P

MESH = pl.DeviceIdType.MESH
F32 = jnp.float32
BF16 = jnp.bfloat16
NT = (((1,), (1,)), ((), ()))
TN = (((0,), (0,)), ((), ()))


def column(row, lanes):
    wide = jnp.broadcast_to(row, (128, row.shape[1])).T
    return jnp.concatenate([wide] * (lanes // 128), axis=1)


def kernel(
    M, N,
    hidden, mix, proj_hbm, vw, logz, targets, loss,
    out_hidden, out_proj, out_vocab,
    w, ctx, mix_all, hblk, hrow, htr, logit, lg, tgt,
    cgs, cgr, cgx, xr, own_cg, vgb, vgy, vsum, vout, vin, pg, hss, hsr, own_hs, acc, psend, precv, mgrad,
    w_sem, ctx_s, ctx_f, ctx_r, mix_s, mix_r, hid_s, hid_r, tgt_s, tgt_r,
    cgp_s, cgp_r, cgx_s, cgx_r, vy_s, vy_r, vz_s, vz_r, hs_s, hs_r, ag_s, ag_r, pp_s, pp_r,
):
    K, D, E = w.shape
    T = hidden.shape[0]
    V = vw.shape[1]
    R = D // M
    half = N // 2
    Z = M // 2
    me_t = lax.axis_index("tok")
    me_v = lax.axis_index("voc")
    chip = me_v // 2
    core = me_v % 2
    partner = me_v + 1 - 2 * core
    z = me_t // 2
    y = me_t % 2
    ypart = me_t + 1 - 2 * y
    sends = []

    def remote(src, dst, ss, rs, dev):
        return pltpu.make_async_remote_copy(
            src_ref=src, dst_ref=dst, send_sem=ss, recv_sem=rs,
            device_id=dev, device_id_type=MESH,
        )

    def send(src, dst, ss, rs, dev):
        c = remote(src, dst, ss, rs, dev)
        c.start()
        sends.append((None, c))

    def arrived(ref, rs, ss):
        remote(ref, ref, ss, rs, {"voc": partner}).wait_recv()

    for k in range(K):
        pltpu.make_async_copy(proj_hbm.at[k], w.at[k], w_sem.at[k]).start()
    for j in range(M):
        hblk[j // 2, j % 2] = hidden[:, j * R:(j + 1) * R]

    bar = pltpu.get_barrier_semaphore()
    for d in range(1, M):
        pl.semaphore_signal(bar, inc=1, device_id={"tok": lax.rem(me_t + d, M)}, device_id_type=MESH)
    for d in range(1, N):
        pl.semaphore_signal(bar, inc=1, device_id={"voc": lax.rem(me_v + d, N)}, device_id_type=MESH)
    pl.semaphore_wait(bar, M + N - 2)

    for d in range(1, N):
        send(mix, mix_all.at[d], mix_s.at[d], mix_r.at[d], {"voc": lax.rem(me_v + d, N)})
    mix_all[0] = mix[...]
    for d in range(1, Z):
        zz = lax.rem(z + d, Z)
        send(hblk.at[zz], hrow.at[:, pl.ds(z * T, T)], hid_s.at[d], hid_r.at[d],
             {"tok": zz * 2 + y})
    hrow[:, rows_of(z, T), :] = hblk[z]

    for k in range(K):
        pltpu.make_async_copy(proj_hbm.at[k], w.at[k], w_sem.at[k]).wait()
        ctx[me_v, k * T:(k + 1) * T, :] = jnp.tanh(
            jnp.dot(hidden[...], w[k], preferred_element_type=F32)
        ).astype(BF16)
        piece = ctx.at[me_v, pl.ds(k * T, T)]
        for i in range(1, half):
            send(piece, piece, ctx_s.at[i, k], ctx_r.at[me_v, k],
                 {"voc": lax.rem(chip + i, half) * 2 + core})
        send(piece, piece, ctx_s.at[0, k], ctx_r.at[me_v, k], {"voc": partner})

    def add_logits(s, first=False):
        part = jnp.dot(ctx[s], vw[pl.ds(pl.multiple_of(s * E, E), E), :],
                       preferred_element_type=F32)
        logit[...] = part if first else logit[...] + part

    add_logits(me_v, True)
    for k in range(K):
        arrived(ctx.at[partner, pl.ds(k * T, T)], ctx_r.at[partner, k], ctx_s.at[0, k])
    add_logits(partner)

    tcol = column(targets[...].astype(F32), V)
    ids = (me_v * V + lax.broadcasted_iota(jnp.int32, (T, V), 1)).astype(F32)
    onehot = (tcol == ids).astype(F32)
    for d in range(1, N):
        arrived(mix_all.at[d], mix_r.at[d], mix_s.at[d])
    mixing = jnp.zeros((K, T), F32)
    for d in range(N):
        s = lax.rem(me_v - d + N, N)
        mixing = mixing + lax.dot_general(
            mix_all[d], hidden[:, pl.ds(pl.multiple_of(s * E, E), E)], NT,
            preferred_element_type=F32)
    exp_mix = jnp.exp(mixing)
    weights = exp_mix / jnp.sum(exp_mix, axis=0, keepdims=True)

    for i in range(1, half):
        s = lax.rem(chip - i + half, half) * 2 + core
        for k in range(K):
            piece = ctx.at[s, pl.ds(k * T, T)]
            arrived(piece, ctx_r.at[s, k], ctx_s.at[i, k])
            send(piece, piece, ctx_f.at[i, k], ctx_r.at[s, k], {"voc": partner})
        add_logits(s)
    for i in range(1, half):
        s = lax.rem(chip - i + half, half) * 2 + 1 - core
        for k in range(K):
            arrived(ctx.at[s, pl.ds(k * T, T)], ctx_r.at[s, k], ctx_s.at[i, k])
        add_logits(s)

    lane = lax.broadcasted_iota(jnp.int32, (T, 128), 1)
    table = jnp.zeros((T, 128), F32)
    for k in range(K):
        part = jnp.sum(logit[k * T:(k + 1) * T, :] * onehot, axis=1, keepdims=True)
        table = jnp.where(lane == k, part, table)
    tgt[0] = table.T[0:8, :]
    for d in range(1, N):
        send(tgt.at[0], tgt.at[d], tgt_s.at[d], tgt_r.at[d], {"voc": lax.rem(me_v + d, N)})
    for k in range(K):
        rows = slice(k * T, (k + 1) * T)
        logit[rows, :] = jnp.exp(logit[rows, :] - column(logz[k:k + 1, :], V)) - onehot
    for d in range(1, N):
        arrived(tgt.at[d], tgt_r.at[d], tgt_s.at[d])
    target = tgt[0]
    for d in range(1, N):
        target = target + tgt[d]
    likely = jnp.exp(target[0:K, :] - logz[...])
    joint = weights * likely
    posterior = joint / jnp.sum(joint, axis=0, keepdims=True)
    factor = loss[...] * posterior
    mgrad[...] = loss[...] * (weights - posterior)
    for k in range(K):
        rows = slice(k * T, (k + 1) * T)
        lg[rows, :] = (column(factor[k:k + 1, :], V) * logit[rows, :]).astype(BF16)

    def cg_part(s, k):
        return lax.dot_general(
            lg[k * T:(k + 1) * T, :], vw[pl.ds(pl.multiple_of(s * E, E), E), :], NT,
            preferred_element_type=F32)

    for i in list(range(1, half)) + [0]:
        s = lax.rem(chip + i, half) * 2
        for k in range(K):
            cgs[i, k] = cg_part(s + 1 - core, k).astype(BF16)
            send(cgs.at[i, k], cgr.at[i, k], cgp_s.at[i, k], cgp_r.at[i, k], {"voc": partner})
        for k in range(K):
            part = cg_part(s + core, k)
            if i == 0:
                own_cg[k] = part
            else:
                arrived(cgr.at[i, k], cgp_r.at[i, k], cgp_s.at[i, k])
                cgx[i, k] = (part + cgr[i, k].astype(F32)).astype(BF16)
                send(cgx.at[i, k], xr.at[i, k], cgx_s.at[i, k], cgx_r.at[i, k], {"voc": s + core})

    for s in range(N):
        vgb[s * E:(s + 1) * E, :] = lax.dot_general(
            ctx[s], lg[...], TN, preferred_element_type=F32).astype(BF16)
    for zz in range(Z):
        send(vgb.at[pl.ds((zz * 2 + 1 - y) * R, R)], vgy.at[zz], vy_s.at[zz], vy_r.at[zz],
             {"tok": ypart})

    for d in range(1, Z):
        src = lax.rem(z - d + Z, Z)
        arrived(hrow.at[:, pl.ds(src * T, T)], hid_r.at[d], hid_s.at[d])
    for b in range(2):
        htr[b] = hrow[b].T

    pieces = [(k, 0, E) for k in range(K)]
    if E % 256 == 0:
        pieces[-1:] = [(K - 1, 0, E // 2), (K - 1, E // 2, E // 2)]

    def relay(t, p, way, pred):
        k, lo, wide = pieces[p]
        piece = pg.at[k, rows_of(t, T), pl.ds(lo, wide)]
        c = remote(piece, piece, ag_s.at[way, t, p], ag_r.at[t, p],
                   {"tok": me_t + 2 - 4 * way})
        pl.when(pred)(c.start)
        sends.append((pred, c))

    has_r = z + 1 < Z
    has_l = z >= 1
    for k in range(K):
        total = own_cg[k]
        arrived(cgr.at[0, k], cgp_r.at[0, k], cgp_s.at[0, k])
        total = total + cgr[0, k].astype(F32)
        for i in range(1, half):
            arrived(xr.at[i, k], cgx_r.at[i, k], cgx_s.at[i, k])
            total = total + xr[i, k].astype(F32)
        c = ctx[me_v, k * T:(k + 1) * T, :].astype(F32)
        pg[k, rows_of(z, T), :] = (total * (1.0 - c * c)).astype(BF16)
        if Z > 1:
            for p in range(len(pieces)):
                if pieces[p][0] == k:
                    relay(z, p, 0, has_r)
                    relay(z, p, 1, has_l)

    def hid_part(s):
        total = jnp.zeros((T, E), F32)
        for k in range(K):
            total = total + lax.dot_general(
                pg[k, rows_of(z, T), :], w[k, pl.ds(pl.multiple_of(s * E, E), E), :], NT,
                preferred_element_type=F32)
        return total

    def hid_send(d):
        s = lax.rem(me_v + d, N)
        if d == 0:
            own_hs[...] = hid_part(s)
        else:
            hss[d] = hid_part(s).astype(BF16)
            send(hss.at[d], hsr.at[d], hs_s.at[d], hs_r.at[d], {"voc": s})

    hid_order = list(range(1, N)) + [0]
    hid_per = -(-N // (len(pieces) - 1))

    def pair_sums():
        for zz in range(Z):
            arrived(vgy.at[zz], vy_r.at[zz], vy_s.at[zz])
            vsum[zz] = vgb[rows_of(zz * 2 + y, R), :].astype(F32) + vgy[zz].astype(F32)

    def hop(h):
        for way, at, ends in ((0, h, range(h + 1, Z)), (1, Z - 1 - h, range(Z - 1 - h))):
            copies = [
                remote(vout.at[way, e], vin.at[way, e], vz_s.at[way, e], vz_r.at[way, e],
                       {"tok": me_t + 2 - 4 * way})
                for e in ends
            ]

            @pl.when(z == at)
            def _(way=way, ends=ends, copies=copies):
                for e, c in zip(ends, copies):
                    part = vsum[e]
                    if h > 0:
                        arrived(vin.at[way, e], vz_r.at[way, e], vz_s.at[way, e])
                        part = part + vin[way, e].astype(F32)
                    vout[way, e] = part.astype(BF16)
                    c.start()
            for c in copies:
                sends.append((z == at, c))

    if Z == 1:
        for e in hid_order:
            hid_send(e)
    per = -(-(Z - 1) // (len(pieces) - 1))
    for p, (k, lo, wide) in enumerate(pieces):
        lanes = slice(lo, lo + wide)
        for d in range(1, Z):
            for there, t, way, more in (
                (z >= d, z - d, 0, has_r), (z + d < Z, z + d, 1, has_l),
            ):
                def _(t=t):
                    arrived(pg.at[k, rows_of(t, T), pl.ds(lo, wide)], ag_r.at[t, p], ag_s.at[0, t, p])
                pl.when(there)(_)
                if d < Z - 1:
                    relay(t, p, way, there & more)
            if d == 1:
                for e in hid_order[p * hid_per:(p + 1) * hid_per]:
                    hid_send(e)
        psend[k, :, lanes] = jnp.dot(
            htr[1 - y], pg[k, :, lanes], preferred_element_type=F32).astype(BF16)
        send(psend.at[k, :, pl.ds(lo, wide)], precv.at[k, :, pl.ds(lo, wide)],
             pp_s.at[p], pp_r.at[p], {"tok": ypart})
        acc[k, :, lanes] = jnp.dot(htr[y], pg[k, :, lanes], preferred_element_type=F32)
        if p == 0:
            pair_sums()
        for h in range(p * per, min((p + 1) * per, Z - 1)):
            hop(h)

    acc_v = vsum.at[z]
    for way, pred in ((0, has_l), (1, has_r)):
        @pl.when(pred)
        def _(way=way):
            arrived(vin.at[way, z], vz_r.at[way, z], vz_s.at[way, z])
            acc_v[...] += vin[way, z].astype(F32)
    out_vocab[...] = acc_v[...].astype(BF16)
    htot = own_hs[...]
    for d in range(1, N):
        arrived(hsr.at[d], hs_r.at[d], hs_s.at[d])
        htot = htot + hsr[d].astype(F32)
    mixf = mix[...].astype(F32)
    for k in range(K):
        htot = htot + column(mgrad[k:k + 1, :], E) * mixf[k:k + 1, :]
    out_hidden[...] = htot.astype(BF16)

    for p, (k, lo, wide) in enumerate(pieces):
        lanes = slice(lo, lo + wide)
        arrived(precv.at[k, :, pl.ds(lo, wide)], pp_r.at[p], pp_s.at[p])
        out_proj[k, :, lanes] = (acc[k, :, lanes] + precv[k, :, lanes].astype(F32)).astype(BF16)
    for pred, c in sends:
        if pred is None:
            c.wait_send()
        else:
            pl.when(pred)(c.wait_send)


def rows_of(block, size):
    return pl.ds(pl.multiple_of(block * size, size), size)


def body(M, N, hidden, mix_weight, comp_proj, vocab_weight, log_normalizer, targets, loss_grad):
    T, D = hidden.shape
    K, E = mix_weight.shape
    V = vocab_weight.shape[1]
    R = D // M
    half = N // 2
    Z = M // 2
    w = jnp.transpose(comp_proj, (1, 0, 2))
    vm = pltpu.VMEM
    dma = pltpu.SemaphoreType.DMA
    scratch = [
        vm((K, D, E), BF16), vm((N, K * T, E), BF16), vm((N, K, E), BF16),
        vm((Z, 2, T, R), BF16), vm((2, Z * T, R), BF16), vm((2, R, Z * T), BF16), vm((K * T, V), F32), vm((K * T, V), BF16),
        vm((N, 8, T), F32),
        vm((half, K, T, E), BF16), vm((half, K, T, E), BF16),
        vm((half, K, T, E), BF16), vm((half, K, T, E), BF16),
        vm((K, T, E), F32), vm((D, V), BF16), vm((Z, R, V), BF16),
        vm((Z, R, V), F32), vm((2, Z, R, V), BF16), vm((2, Z, R, V), BF16),
        vm((K, Z * T, E), BF16), vm((N, T, E), BF16), vm((N, T, E), BF16),
        vm((T, E), F32), vm((K, R, E), F32), vm((K, R, E), BF16), vm((K, R, E), BF16),
        vm((K, T), F32),
        dma((K,)), dma((half, K)), dma((half, K)), dma((N, K)), dma((N,)), dma((N,)),
        dma((Z,)), dma((Z,)), dma((N,)), dma((N,)),
        dma((half, K)), dma((half, K)), dma((half, K)), dma((half, K)),
        dma((Z,)), dma((Z,)), dma((2, Z)), dma((2, Z)), dma((N,)), dma((N,)),
        dma((2, Z, K + 1)), dma((Z, K + 1)), dma((K + 1,)), dma((K + 1,)),
    ]
    spec = pl.BlockSpec(memory_space=pltpu.VMEM)
    hidden_grad, proj_grad, vocab_grad = pl.pallas_call(
        functools.partial(kernel, M, N),
        out_shape=(
            jax.ShapeDtypeStruct((T, E), BF16),
            jax.ShapeDtypeStruct((K, R, E), BF16),
            jax.ShapeDtypeStruct((R, V), BF16),
        ),
        in_specs=[spec, spec, pl.BlockSpec(memory_space=pltpu.MemorySpace.HBM)] + [spec] * 4,
        out_specs=(spec, spec, spec),
        scratch_shapes=scratch,
        compiler_params=pltpu.CompilerParams(
            collective_id=0, has_side_effects=True, vmem_limit_bytes=48 * 1024 * 1024
        ),
    )(hidden, mix_weight, w, vocab_weight, log_normalizer, targets[None, :], loss_grad[None, :])
    return hidden_grad, jnp.transpose(proj_grad, (1, 0, 2)), vocab_grad


def solution(mesh):
    in_specs = (
        P("tok", None),
        P(None, "voc"),
        P(None, None, "voc"),
        P(None, "voc"),
        P(None, "tok"),
        P("tok"),
        P("tok"),
    )
    out_specs = (P("tok", "voc"), P("tok", None, "voc"), P("tok", "voc"))
    return jax.shard_map(
        functools.partial(body, mesh.shape["tok"], mesh.shape["voc"]),
        mesh=mesh, in_specs=in_specs, out_specs=out_specs, check_vma=False,
    )
```
